32 devices in a mesh: gx: 4 (over y, x), gy: 2 (over core), gz: 4 (over z).
Axes of the slice: x: 2, y: 2, z: 4, core: 2. Of those that a mesh axis runs over, the one named last changes fastest.
Arguments:
- populations: float32 [2, 19, 16, 32, 512], P(None, None, 'gx', 'gy', 'gz'), may hold values from 0.01 to 0.2
- solid: int32 [16, 32, 512], P('gx', 'gy', 'gz'), may hold values 0 or 1
Outputs:
- read: float32 [2, 19, 16, 32, 512], P(None, None, 'gx', 'gy', 'gz')
The draws below stay inside these ranges and needn't reach their ends.
All inputs are finite; a program needn't handle non-finite values. No bound on the sum of `solid` on one device may be relied on, other than what follows from the above.
Results may differ from the reference program's by a relative error of at most 0.0001.
Values sent between devices are 32-bit elements; how exact they have to be, the bound alone decides.
A program may use at most 64 MiB of HBM per device.

```python
import math
import jax
import jax.numpy as jnp
import numpy as np
from jax import lax

NX = 16
NY = 32
NZ = 512


def touch_ends(values, own_key, smallest, high):
    extent = values.shape
    index_at = [jax.random.randint(jax.random.fold_in(own_key, axis), (), 0, extent[axis]) for axis in range(len(extent))]
    values = values.at[tuple(index_at)].set(smallest)
    longest = extent.index(max(extent))
    index_at[longest] = (index_at[longest] + 1) % extent[longest]
    return values.at[tuple(index_at)].set(high)


def steps_of(own_key, extent, shards, least, top_value):
    factor_of, own = 1.0, jax.random.fold_in(own_key, 6)
    for dim, blocks in shards:
        steps = jnp.exp(jax.random.uniform(jax.random.fold_in(own, dim), (blocks,), jnp.float32, least / len(shards), top_value / len(shards)))
        factor_of = factor_of * jnp.repeat(steps, extent[dim] // blocks).reshape([-1 if axis == dim else 1 for axis in range(len(extent))])
    return factor_of


def setup_inputs(seed: int = 0) -> dict:
    key_of = jax.random.split(jax.random.key(seed), 3)
    return {
        "populations": jnp.clip(jnp.exp(math.log(0.2) - 2.9957323 * jax.random.uniform(key_of[0], (2, 19, NX, NY, NZ), jnp.float32) ** steps_of(key_of[0], (2, 19, NX, NY, NZ), ((2, 4), (3, 2), (4, 4)), -0.2, 0.2)), 0.01, 0.2),
        "solid": touch_ends((jax.random.randint(key_of[1], (NX, NY, NZ), 0, 8) < 1).astype(jnp.int32), jax.random.fold_in(key_of[1], 1), 0, 1),
    }


VELOCITIES = [(0, 0, 0), (1, 0, 0), (-1, 0, 0), (0, 1, 0), (0, -1, 0), (0, 0, 1), (0, 0, -1),
              (1, 1, 0), (-1, -1, 0), (1, -1, 0), (-1, 1, 0), (1, 0, 1), (-1, 0, -1), (1, 0, -1),
              (-1, 0, 1), (0, 1, 1), (0, -1, -1), (0, 1, -1), (0, -1, 1)]
WEIGHTS = [1.0 / 3.0] + [1.0 / 18.0] * 6 + [1.0 / 36.0] * 12
OPPOSITE = [0, 2, 1, 4, 3, 6, 5, 8, 7, 10, 9, 12, 11, 14, 13, 16, 15, 18, 17]
coupling = 0.9
relax_times = (1.0, 0.8)
wall_values = (0.3, 1.5)


def collide(populations, fluid, psi, gradient):
    vel = jnp.asarray(np.array(VELOCITIES, np.float32))
    weights = jnp.asarray(np.array(WEIGHTS, np.float32))
    rho = jnp.sum(populations, axis=1)
    moment = jnp.einsum("ia,kixyz->kaxyz", vel, populations, precision=lax.Precision.HIGHEST)
    inv_first = 1.0 / relax_times[0]
    inv_second = 1.0 / relax_times[1]
    weight_sum = rho[0] * inv_first + rho[1] * inv_second
    common = (moment[0] * inv_first + moment[1] * inv_second) / weight_sum[None]
    forces = (-coupling * psi[0][None] * gradient[1], -coupling * psi[1][None] * gradient[0])
    results = []
    for comp in range(2):
        velocity = common + relax_times[comp] * forces[comp] / rho[comp][None]
        along = jnp.einsum("ia,axyz->ixyz", vel, velocity, precision=lax.Precision.HIGHEST)
        speed_sq = jnp.sum(velocity * velocity, axis=0)
        equil = weights[:, None, None, None] * rho[comp][None] * (
            1.0 + 3.0 * along + 4.5 * along * along - 1.5 * speed_sq[None])
        current = populations[comp]
        results.append(current - (current - equil) / relax_times[comp])
    post = jnp.stack(results, axis=0)
    return jnp.where(fluid[None, None], post, populations)


def reference(populations, solid):
    fluid = solid == 0
    rho = jnp.sum(populations, axis=1)
    wall = jnp.asarray(np.array(wall_values, np.float32)).reshape(2, 1, 1, 1)
    psi = jnp.where(fluid[None], rho, wall)
    parts = [jnp.zeros_like(psi) for axis_idx in range(3)]
    for i in range(1, 19):
        move = VELOCITIES[i]
        shifted = jnp.roll(psi, (-move[0], -move[1], -move[2]), axis=(1, 2, 3))
        for axis_idx in range(3):
            if move[axis_idx] != 0:
                parts[axis_idx] = parts[axis_idx] + (WEIGHTS[i] * move[axis_idx]) * shifted
    gradient = jnp.stack(parts, axis=1)
    post = collide(populations, fluid, psi, gradient)
    moved = []
    for i in range(19):
        move = VELOCITIES[i]
        pulled = jnp.roll(post[:, i], move, axis=(1, 2, 3))
        source_fluid = jnp.roll(fluid, move, axis=(0, 1, 2))
        moved.append(jnp.where(source_fluid[None], pulled, post[:, OPPOSITE[i]]))
    result = jnp.stack(moved, axis=1)
    return jnp.where(fluid[None, None], result, populations)
```

```python
import jax
import jax.numpy as jnp
from jax import lax
from jax.experimental import pallas as pl
from jax.experimental.pallas import tpu as pltpu
from jax.sharding import PartitionSpec as P

VELOCITIES = [
    (0, 0, 0),
    (1, 0, 0),
    (-1, 0, 0),
    (0, 1, 0),
    (0, -1, 0),
    (0, 0, 1),
    (0, 0, -1),
    (1, 1, 0),
    (-1, -1, 0),
    (1, -1, 0),
    (-1, 1, 0),
    (1, 0, 1),
    (-1, 0, -1),
    (1, 0, -1),
    (-1, 0, 1),
    (0, 1, 1),
    (0, -1, -1),
    (0, 1, -1),
    (0, -1, 1),
]
WEIGHTS = [1.0 / 3.0] + [1.0 / 18.0] * 6 + [1.0 / 36.0] * 12
OPPOSITE = [0, 2, 1, 4, 3, 6, 5, 8, 7, 10, 9, 12, 11, 14, 13, 16, 15, 18, 17]
COUPLING = 0.9
RELAX = (1.0, 0.8)
WALL = (0.3, 1.5)
AXES = ("gx", "gy", "gz")
MESH = pl.DeviceIdType.MESH

ORDER = (
    [0]
    + [i for i in range(19) if VELOCITIES[i][0] == 1]
    + [i for i in range(19) if VELOCITIES[i][0] == -1]
    + [i for i in range(1, 19) if VELOCITIES[i][0] == 0]
)
SLOT = {i: s for s, i in enumerate(ORDER)}
Z_UP = [i for i in range(19) if VELOCITIES[i][2] == 1]
Z_PAIR = {}
for _g, _i in enumerate(Z_UP):
    Z_PAIR[_i] = _g
    Z_PAIR[OPPOSITE[_i]] = _g
Z_OFFSETS = [v for v in VELOCITIES if v[2] != 0]
Z_INDEX = {v: n for n, v in enumerate(Z_OFFSETS)}
T = 8
LANES = 128


def step_kernel(pop_hbm, solid_hbm, out_hbm, pop, solid, out, psi, zpsi, post, zpost, vel, source,
                pack1, recv1, pack2, recv2, load_sem, store_sem, send1, got1, send2, got2):
    X, Y, Z = solid.shape
    YT = Y // T
    lo, hi = slice(T, 2 * T), slice(Y, Y + T)
    low_halo, high_halo = slice(0, T), slice(Y + T, Y + 2 * T)
    inner = slice(T, Y + T)

    loads = [pltpu.make_async_copy(solid_hbm, solid, load_sem.at[X])]
    loads += [
        pltpu.make_async_copy(pop_hbm.at[:, :, x], pop.at[:, :, x], load_sem.at[x])
        for x in range(X)
    ]
    for copy in loads:
        copy.start()

    me = [lax.axis_index(a) for a in AXES]
    count = [lax.axis_size(a) for a in AXES]

    def device(offset):
        return tuple(lax.rem(me[d] + offset[d] + count[d], count[d]) for d in range(3))

    barrier = pltpu.get_barrier_semaphore()
    for offset in VELOCITIES[1:]:
        pl.semaphore_signal(barrier, inc=1, device_id=device(offset), device_id_type=MESH)

    lane = lax.broadcasted_iota(jnp.int32, (T, LANES), 1)
    pair = lane // 2
    lane_y = lax.broadcasted_iota(jnp.int32, (Y, LANES), 1)
    first, last = lane_y == 0, lane_y == Z - 1

    loads[0].wait()
    inv = [1.0 / t for t in RELAX]
    packed = jnp.zeros((T, LANES), jnp.float32)

    def combo1(k, x, t):
        return (k * X + x) * YT + t

    for x in range(X):
        loads[1 + x].wait()
        fluid = solid[x] == 0
        total, mom = [], [[], [], []]
        for k in range(2):
            f = [pop[k, i, x] for i in range(19)]
            rho = f[0]
            m = [None, None, None]
            for i in range(1, 19, 2):
                rho = rho + (f[i] + f[i + 1])
                diff = f[i] - f[i + 1]
                for d in range(3):
                    c = VELOCITIES[i][d]
                    if c:
                        m[d] = (
                            (diff if c > 0 else -diff)
                            if m[d] is None
                            else (m[d] + diff if c > 0 else m[d] - diff)
                        )
            total.append(rho)
            signed = jnp.where(fluid, rho, -WALL[k])
            psi[k, 1 + x, inner] = signed
            for d in range(3):
                mom[d].append(m[d] * inv[k] if inv[k] != 1.0 else m[d])
            for t in range(YT):
                j = combo1(k, x, t)
                piece = pltpu.roll(signed[t * T:(t + 1) * T], (2 * j + 1) % LANES, 1)
                packed = jnp.where(pair == j, piece, packed)
        scale = 1.0 / (total[0] * inv[0] + total[1] * inv[1])
        for d in range(3):
            vel[d, x] = (mom[d][0] + mom[d][1]) * scale
    pack1[...] = packed

    pl.semaphore_wait(barrier, 18)

    def remote(src, dst, send, recv, n, offset):
        return pltpu.make_async_remote_copy(
            src_ref=src,
            dst_ref=dst,
            send_sem=send.at[n],
            recv_sem=recv.at[n],
            device_id=device(offset),
            device_id_type=MESH,
        )

    def edge_of(offset):
        dx, dy, _ = offset
        src_x = slice(1, X + 1) if dx == 0 else (slice(X, X + 1) if dx > 0 else slice(1, 2))
        dst_x = slice(1, X + 1) if dx == 0 else (slice(0, 1) if dx > 0 else slice(X + 1, X + 2))
        src_y = inner if dy == 0 else (hi if dy > 0 else lo)
        dst_y = inner if dy == 0 else (low_halo if dy > 0 else high_halo)
        return (src_x, src_y), (dst_x, dst_y)

    order = sorted(range(1, 19), key=lambda i: -sum(abs(c) for c in VELOCITIES[i][::2]))
    copies1 = []
    for n, i in enumerate(order):
        offset = VELOCITIES[i]
        if offset[2]:
            copy = remote(pack1, recv1.at[Z_INDEX[offset]], send1, got1, n, offset)
        else:
            s, d = edge_of(offset)
            copy = remote(psi.at[:, s[0], s[1]], psi.at[:, d[0], d[1]], send1, got1, n, offset)
        copy.start()
        copies1.append(copy)
    for copy in copies1:
        copy.wait_recv()

    def came1(x, y, z):
        return recv1[Z_INDEX[(-x, -y, -z)]]

    def put1(merged, k, x, t, plane, rows):
        zpsi[k, plane, rows] = pltpu.roll(merged, (LANES - 2 * combo1(k, x, t) - 1) % LANES, 1)

    even = lane % 2 == 0
    for dx, dy in ((0, 0), (-1, 0), (1, 0), (0, -1), (0, 1)):
        merged = jnp.where(even, came1(dx, dy, -1), came1(dx, dy, 1))
        xs = range(X) if dx == 0 else ([X - 1] if dx < 0 else [0])
        ts = range(YT) if dy == 0 else ([YT - 1] if dy < 0 else [0])
        for k in range(2):
            for x in xs:
                for t in ts:
                    plane = 1 + x + dx * X
                    row = T * (1 + t + dy * YT)
                    put1(merged, k, x, t, plane, slice(row, row + T))

    def shifted(base, edge, move):
        if move[2] == 0:
            return base
        if move[2] > 0:
            return pltpu.roll(jnp.where(first, edge, base), Z - 1, 1)
        return pltpu.roll(jnp.where(last, edge, base), 1, 1)

    half = X // 2

    def combo2(k, g, x, t):
        return (((x % half) * 2 + k) * 5 + g) * YT + t

    packs = [jnp.zeros((T, LANES), jnp.float32) for _ in range(2)]
    for x in range(X):
        grads = []
        for k in range(2):
            parts = [None, None, None]
            beside = {}
            for i in range(1, 19):
                c = VELOCITIES[i]
                at = (k, 1 + x + c[0], slice(T + c[1], T + c[1] + Y))
                value = shifted(psi[at], zpsi[at] if c[2] else None, c)
                if k == 0:
                    source[OPPOSITE[i], x] = value
                beside[i] = jnp.abs(value)
            for i in range(1, 19, 2):
                term = WEIGHTS[i] * (beside[i] - beside[i + 1])
                for d in range(3):
                    c = VELOCITIES[i][d]
                    if c:
                        parts[d] = (
                            (term if c > 0 else -term)
                            if parts[d] is None
                            else (parts[d] + term if c > 0 else parts[d] - term)
                        )
            grads.append(parts)
        for k in range(2):
            u = [vel[d, x] - (COUPLING * RELAX[k]) * grads[1 - k][d] for d in range(3)]
            rho = jnp.abs(psi[k, 1 + x, inner]) * inv[k]
            rest = 1.0 - inv[k]
            flat = 1.0 - 1.5 * (u[0] * u[0] + u[1] * u[1] + u[2] * u[2])
            keep = 1.0 - inv[k]
            rho_w = {w: rho * w for w in set(WEIGHTS)}
            values = {}

            def finish(i, eq):
                if abs(keep) > 1e-9:
                    eq = eq + keep * pop[k, i, x]
                post[k, SLOT[i], 1 + x, inner] = eq
                values[i] = eq

            finish(0, rho_w[WEIGHTS[0]] * flat)
            for i in range(1, 19, 2):
                along = None
                for d in range(3):
                    c = VELOCITIES[i][d]
                    if c:
                        along = (
                            (u[d] if c > 0 else -u[d])
                            if along is None
                            else (along + u[d] if c > 0 else along - u[d])
                        )
                w = rho_w[WEIGHTS[i]]
                even_part = w * (flat + 4.5 * (along * along))
                odd_part = w * (3.0 * along)
                finish(i, even_part + odd_part)
                finish(i + 1, even_part - odd_part)
            for g, i in enumerate(Z_UP):
                ends = jnp.where(last, values[i], values[OPPOSITE[i]])
                for t in range(YT):
                    j = combo2(k, g, x, t)
                    piece = pltpu.roll(ends[t * T:(t + 1) * T], (2 * j + 1) % LANES, 1)
                    packs[x // half] = jnp.where(pair == j, piece, packs[x // half])
    for h in range(2):
        pack2[h] = packs[h]

    copies2 = []

    def launch2(src, dst, offset):
        copy = remote(src, dst, send2, got2, len(copies2), offset)
        copy.start()
        copies2.append(copy)

    for i in order:
        offset = VELOCITIES[i]
        if offset[2]:
            halves = slice(0, 2) if offset[0] == 0 else (slice(1, 2) if offset[0] > 0 else slice(0, 1))
            launch2(pack2.at[halves], recv2.at[Z_INDEX[offset], halves], offset)
            continue
        s, d = edge_of(offset)
        if offset[0] and offset[1]:
            launch2(post.at[:, SLOT[i], s[0], s[1]], post.at[:, SLOT[i], d[0], d[1]], offset)
        elif offset[0]:
            group = slice(1, 6) if offset[0] > 0 else slice(6, 11)
            launch2(post.at[:, group, s[0], s[1]], post.at[:, group, d[0], d[1]], offset)
        else:
            for q in range(19):
                if VELOCITIES[q][1] == offset[1]:
                    launch2(post.at[:, SLOT[q], s[0], s[1]], post.at[:, SLOT[q], d[0], d[1]], offset)

    for x in range(X):
        fluid = solid[x] == 0
        for k in range(2):
            out[k, 0, x] = jnp.where(fluid, post[k, 0, 1 + x, inner], pop[k, 0, x])

    for copy in copies2:
        copy.wait_recv()

    def came2(x, y, z, h):
        return recv2[Z_INDEX[(-x, -y, -z)], h]

    def put2(tile, k, g, x, t, plane, rows):
        zpost[k, g, plane, rows] = pltpu.roll(tile, (LANES - 2 * combo2(k, g, x, t) - 1) % LANES, 1)

    for h in range(2):
        merged = jnp.where(even, came2(0, 0, -1, h), came2(0, 0, 1, h))
        for x in range(h * half, (h + 1) * half):
            for k in range(2):
                for g in range(5):
                    for t in range(YT):
                        row = T * (1 + t)
                        put2(merged, k, g, x, t, 1 + x, slice(row, row + T))
    for i in range(1, 19):
        c = VELOCITIES[i]
        if c[2] == 0 or (c[0] == 0 and c[1] == 0):
            continue
        g = Z_PAIR[i]
        for k in range(2):
            if c[0]:
                x = X - 1 if c[0] > 0 else 0
                plane = 0 if c[0] > 0 else X + 1
                for t in range(YT):
                    row = T * (1 + t)
                    put2(came2(-c[0], 0, -c[2], x // half), k, g, x, t, plane, slice(row, row + T))
            else:
                t = YT - 1 if c[1] > 0 else 0
                rows = low_halo if c[1] > 0 else high_halo
                for x in range(X):
                    put2(came2(0, -c[1], -c[2], x // half), k, g, x, t, 1 + x, rows)

    stores = []
    for x in range(X):
        fluid = solid[x] == 0
        for k in range(2):
            for i in range(1, 19):
                c = VELOCITIES[i]
                back = tuple(-a for a in c)
                rows = slice(T - c[1], T - c[1] + Y)
                base = post[k, SLOT[i], 1 + x - c[0], rows]
                edge = zpost[k, Z_PAIR[i], 1 + x - c[0], rows] if c[2] else None
                pulled = shifted(base, edge, back)
                bounced = post[k, SLOT[OPPOSITE[i]], 1 + x, inner]
                read = jnp.where(source[i, x] > 0.0, pulled, bounced)
                out[k, i, x] = jnp.where(fluid, read, pop[k, i, x])
        copy = pltpu.make_async_copy(out.at[:, :, x], out_hbm.at[:, :, x], store_sem.at[x])
        copy.start()
        stores.append(copy)
    for copy in copies1 + copies2:
        copy.wait_send()
    for copy in stores:
        copy.wait()


def body(populations, solid):
    X, Y, Z = solid.shape
    f32 = jnp.float32
    dma = pltpu.SemaphoreType.DMA
    return pl.pallas_call(
        step_kernel,
        out_shape=jax.ShapeDtypeStruct(populations.shape, f32),
        in_specs=[pl.BlockSpec(memory_space=pl.ANY)] * 2,
        out_specs=pl.BlockSpec(memory_space=pl.ANY),
        scratch_shapes=[
            pltpu.VMEM(populations.shape, f32),
            pltpu.VMEM(solid.shape, jnp.int32),
            pltpu.VMEM(populations.shape, f32),
            pltpu.VMEM((2, X + 2, Y + 2 * T, Z), f32),
            pltpu.VMEM((2, X + 2, Y + 2 * T, Z), f32),
            pltpu.VMEM((2, 19, X + 2, Y + 2 * T, Z), f32),
            pltpu.VMEM((2, 5, X + 2, Y + 2 * T, Z), f32),
            pltpu.VMEM((3, X, Y, Z), f32),
            pltpu.VMEM((19, X, Y, Z), f32),
            pltpu.VMEM((T, LANES), f32),
            pltpu.VMEM((10, T, LANES), f32),
            pltpu.VMEM((2, T, LANES), f32),
            pltpu.VMEM((10, 2, T, LANES), f32),
            dma((X + 1,)),
            dma((X,)),
            dma((18,)),
            dma((18,)),
            dma((26,)),
            dma((26,)),
        ],
        compiler_params=pltpu.CompilerParams(collective_id=0, has_side_effects=True),
    )(populations, solid)


def solution(mesh):
    in_specs = (P(None, None, "gx", "gy", "gz"), P("gx", "gy", "gz"))
    out_specs = P(None, None, "gx", "gy", "gz")
    return jax.shard_map(body, mesh=mesh, in_specs=in_specs, out_specs=out_specs, check_vma=False)
```

```python
import jax
import jax.numpy as jnp
from jax import lax
from jax.experimental import pallas as pl
from jax.experimental.pallas import tpu as pltpu
from jax.sharding import PartitionSpec as P

VELOCITIES = [
    (0, 0, 0),
    (1, 0, 0),
    (-1, 0, 0),
    (0, 1, 0),
    (0, -1, 0),
    (0, 0, 1),
    (0, 0, -1),
    (1, 1, 0),
    (-1, -1, 0),
    (1, -1, 0),
    (-1, 1, 0),
    (1, 0, 1),
    (-1, 0, -1),
    (1, 0, -1),
    (-1, 0, 1),
    (0, 1, 1),
    (0, -1, -1),
    (0, 1, -1),
    (0, -1, 1),
]
WEIGHTS = [1.0 / 3.0] + [1.0 / 18.0] * 6 + [1.0 / 36.0] * 12
OPPOSITE = [0, 2, 1, 4, 3, 6, 5, 8, 7, 10, 9, 12, 11, 14, 13, 16, 15, 18, 17]
COUPLING = 0.9
RELAX = (1.0, 0.8)
WALL = (0.3, 1.5)
AXES = ("gx", "gy", "gz")
MESH = pl.DeviceIdType.MESH

ORDER = (
    [0]
    + [i for i in range(19) if VELOCITIES[i][0] == 1]
    + [i for i in range(19) if VELOCITIES[i][0] == -1]
    + [i for i in range(1, 19) if VELOCITIES[i][0] == 0]
)
SLOT = {i: s for s, i in enumerate(ORDER)}
Z_UP = [i for i in range(19) if VELOCITIES[i][2] == 1]
Z_PAIR = {}
for _g, _i in enumerate(Z_UP):
    Z_PAIR[_i] = _g
    Z_PAIR[OPPOSITE[_i]] = _g
Z_OFFSETS = [v for v in VELOCITIES if v[2] != 0]
Z_INDEX = {v: n for n, v in enumerate(Z_OFFSETS)}
T = 8
LANES = 128


def step_kernel(pop_hbm, solid_hbm, out, pop, solid, psi, zpsi, post, zpost, vel, source,
                pack1, recv1, pack2, recv2, face, ghost, load_sem, send1, got1, send2, got2):
    X, Y, Z = solid.shape
    YT = Y // T
    lo, hi = slice(T, 2 * T), slice(Y, Y + T)
    low_halo, high_halo = slice(0, T), slice(Y + T, Y + 2 * T)
    inner = slice(T, Y + T)

    loads = [pltpu.make_async_copy(solid_hbm, solid, load_sem.at[X])]
    loads += [
        pltpu.make_async_copy(pop_hbm.at[:, :, x], pop.at[:, :, x], load_sem.at[x])
        for x in range(X)
    ]
    for copy in loads:
        copy.start()

    me = [lax.axis_index(a) for a in AXES]
    count = [lax.axis_size(a) for a in AXES]

    def device(offset):
        return tuple(lax.rem(me[d] + offset[d] + count[d], count[d]) for d in range(3))

    barrier = pltpu.get_barrier_semaphore()
    greeted = [v for v in VELOCITIES[1:] if not (v[0] and v[2])]
    for offset in greeted:
        pl.semaphore_signal(barrier, inc=1, device_id=device(offset), device_id_type=MESH)

    lane = lax.broadcasted_iota(jnp.int32, (T, LANES), 1)
    pair = lane // 2
    lane_y = lax.broadcasted_iota(jnp.int32, (Y, LANES), 1)
    first, last = lane_y == 0, lane_y == Z - 1

    loads[0].wait()
    inv = [1.0 / t for t in RELAX]
    packed = jnp.zeros((T, LANES), jnp.float32)

    def combo1(k, x, t):
        return (k * X + x) * YT + t

    for x in range(X):
        loads[1 + x].wait()
        fluid = solid[x] == 0
        total, mom = [], [[], [], []]
        for k in range(2):
            f = [pop[k, i, x] for i in range(19)]
            rho = f[0]
            m = [None, None, None]
            for i in range(1, 19, 2):
                rho = rho + (f[i] + f[i + 1])
                diff = f[i] - f[i + 1]
                for d in range(3):
                    c = VELOCITIES[i][d]
                    if c:
                        m[d] = (
                            (diff if c > 0 else -diff)
                            if m[d] is None
                            else (m[d] + diff if c > 0 else m[d] - diff)
                        )
            total.append(rho)
            signed = jnp.where(fluid, rho, -WALL[k])
            psi[k, 1 + x, inner] = signed
            for d in range(3):
                mom[d].append(m[d] * inv[k] if inv[k] != 1.0 else m[d])
            for t in range(YT):
                j = combo1(k, x, t)
                piece = pltpu.roll(signed[t * T:(t + 1) * T], (2 * j + 1) % LANES, 1)
                packed = jnp.where(pair == j, piece, packed)
        scale = 1.0 / (total[0] * inv[0] + total[1] * inv[1])
        for d in range(3):
            vel[d, x] = (mom[d][0] + mom[d][1]) * scale
    pack1[...] = packed

    pl.semaphore_wait(barrier, len(greeted))

    def remote(src, dst, send, recv, n, offset):
        return pltpu.make_async_remote_copy(
            src_ref=src,
            dst_ref=dst,
            send_sem=send.at[n],
            recv_sem=recv.at[n],
            device_id=device(offset),
            device_id_type=MESH,
        )

    def edge_of(offset):
        dx, dy, _ = offset
        src_x = slice(1, X + 1) if dx == 0 else (slice(X, X + 1) if dx > 0 else slice(1, 2))
        dst_x = slice(1, X + 1) if dx == 0 else (slice(0, 1) if dx > 0 else slice(X + 1, X + 2))
        src_y = inner if dy == 0 else (hi if dy > 0 else lo)
        dst_y = inner if dy == 0 else (low_halo if dy > 0 else high_halo)
        return (src_x, src_y), (dst_x, dst_y)

    order = sorted(range(1, 19), key=lambda i: -sum(abs(c) for c in VELOCITIES[i][::2]))
    copies1 = {}
    for offset in sorted(greeted, key=lambda v: (-abs(v[2]), abs(v[0]) + abs(v[1]))):
        n = len(copies1)
        if offset[2]:
            copy = remote(pack1, recv1.at[Z_INDEX[offset]], send1, got1, n, offset)
        else:
            s, d = edge_of(offset)
            copy = remote(psi.at[:, s[0], s[1]], psi.at[:, d[0], d[1]], send1, got1, n, offset)
        copy.start()
        copies1[offset] = copy
    raw = []
    for side in (1, -1):
        for i in range(19):
            if VELOCITIES[i][0] == side:
                src_plane, dst_plane = (X - 1, 0) if side > 0 else (0, X + 1)
                copy = remote(pop.at[1, i, src_plane], post.at[1, SLOT[i], dst_plane, inner],
                              send1, got1, 18 + len(raw), (side, 0, 0))
                copy.start()
                raw.append(copy)
    for dz in (1, -1):
        copies1[(0, 0, dz)].wait_recv()
        for dx in (1, -1):
            copy = remote(recv1.at[Z_INDEX[(0, 0, dz)]], recv1.at[Z_INDEX[(dx, 0, dz)]],
                          send1, got1, len(copies1), (dx, 0, 0))
            copy.start()
            copies1[(dx, 0, dz)] = copy
    for offset in greeted:
        if offset[:2] != (0, 0):
            copies1[offset].wait_recv()

    def came1(x, y, z):
        return recv1[Z_INDEX[(-x, -y, -z)]]

    def put1(merged, k, x, t, plane, rows):
        zpsi[k, plane, rows] = pltpu.roll(merged, (LANES - 2 * combo1(k, x, t) - 1) % LANES, 1)

    even = lane % 2 == 0

    def unpack1(dx, dy):
        merged = jnp.where(even, came1(dx, dy, -1), came1(dx, dy, 1))
        xs = range(X) if dx == 0 else ([X - 1] if dx < 0 else [0])
        ts = range(YT) if dy == 0 else ([YT - 1] if dy < 0 else [0])
        for k in range(2):
            for x in xs:
                for t in ts:
                    plane = 1 + x + dx * X
                    row = T * (1 + t + dy * YT)
                    put1(merged, k, x, t, plane, slice(row, row + T))

    for dx, dy in ((0, 0), (0, -1), (0, 1)):
        unpack1(dx, dy)

    def shifted(base, edge, move):
        if move[2] == 0:
            return base
        if move[2] > 0:
            return pltpu.roll(jnp.where(first, edge, base), Z - 1, 1)
        return pltpu.roll(jnp.where(last, edge, base), 1, 1)

    half = X // 2

    def combo2(k, g, x, t):
        return (((x % half) * 2 + k) * 5 + g) * YT + t

    def equilibrium(pairs, rho_of, u):
        flat = 1.0 - 1.5 * (u[0] * u[0] + u[1] * u[1] + u[2] * u[2])
        result = {}
        for i, signs in pairs:
            if i == 0:
                result[0] = rho_of[WEIGHTS[0]] * flat
                continue
            along = None
            for d in range(3):
                c = VELOCITIES[i][d]
                if c:
                    along = (
                        (u[d] if c > 0 else -u[d])
                        if along is None
                        else (along + u[d] if c > 0 else along - u[d])
                    )
            w = rho_of[WEIGHTS[i]]
            even_part = w * (flat + 4.5 * (along * along))
            odd_part = w * (3.0 * along)
            if 1 in signs:
                result[i] = even_part + odd_part
            if -1 in signs:
                result[i + 1] = even_part - odd_part
        return result

    everything = [(0, (1,))] + [(i, (1, -1)) for i in range(1, 19, 2)]
    copies2 = []
    kinds = []

    def launch2(src, dst, offset):
        copy = remote(src, dst, send2, got2, len(copies2), offset)
        copy.start()
        copies2.append(copy)
        kinds.append(tuple(abs(c) for c in offset))

    packs = [jnp.zeros((T, LANES), jnp.float32) for _ in range(2)]
    for x in list(range(1, X - 1)) + [0, X - 1]:
        if x == 0:
            for dx in (1, -1):
                for dz in (1, -1):
                    copies1[(dx, 0, dz)].wait_recv()
            for dx in (1, -1):
                unpack1(dx, 0)
        grads = []
        for k in range(2):
            parts = [None, None, None]
            beside = {}
            for i in range(1, 19):
                c = VELOCITIES[i]
                at = (k, 1 + x + c[0], slice(T + c[1], T + c[1] + Y))
                value = shifted(psi[at], zpsi[at] if c[2] else None, c)
                if k == 0:
                    source[OPPOSITE[i], x] = value
                beside[i] = jnp.abs(value)
            for i in range(1, 19, 2):
                term = WEIGHTS[i] * (beside[i] - beside[i + 1])
                for d in range(3):
                    c = VELOCITIES[i][d]
                    if c:
                        parts[d] = (
                            (term if c > 0 else -term)
                            if parts[d] is None
                            else (parts[d] + term if c > 0 else parts[d] - term)
                        )
            grads.append(parts)
        for k in range(2):
            u = [vel[d, x] - (COUPLING * RELAX[k]) * grads[1 - k][d] for d in range(3)]
            rho = jnp.abs(psi[k, 1 + x, inner]) * inv[k]
            keep = 1.0 - inv[k]
            values = equilibrium(everything, {w: rho * w for w in sorted(set(WEIGHTS))}, u)
            for i in range(19):
                if abs(keep) > 1e-9:
                    values[i] = values[i] + keep * pop[k, i, x]
                post[k, SLOT[i], 1 + x, inner] = values[i]
            if x in (0, X - 1):
                for d in range(3):
                    face[int(x != 0), 3 * k + d] = u[d]
            for g, i in enumerate(Z_UP):
                ends = jnp.where(last, values[i], values[OPPOSITE[i]])
                for t in range(YT):
                    j = combo2(k, g, x, t)
                    piece = pltpu.roll(ends[t * T:(t + 1) * T], (2 * j + 1) % LANES, 1)
                    packs[x // half] = jnp.where(pair == j, piece, packs[x // half])
        if x in (0, X - 1):
            side = int(x != 0)
            launch2(face.at[side], ghost.at[1 - side], (2 * side - 1, 0, 0))
    for h in range(2):
        pack2[h] = packs[h]

    for i in order:
        offset = VELOCITIES[i]
        if offset[2]:
            halves = slice(0, 2) if offset[0] == 0 else (slice(1, 2) if offset[0] > 0 else slice(0, 1))
            launch2(pack2.at[halves], recv2.at[Z_INDEX[offset], halves], offset)
            continue
        s, d = edge_of(offset)
        if offset[0] and offset[1]:
            launch2(post.at[:, SLOT[i], s[0], s[1]], post.at[:, SLOT[i], d[0], d[1]], offset)
        elif offset[1]:
            for q in range(19):
                if VELOCITIES[q][1] == offset[1]:
                    launch2(post.at[:, SLOT[q], s[0], s[1]], post.at[:, SLOT[q], d[0], d[1]], offset)

    def await2(*wanted):
        for copy, kind in zip(copies2, kinds):
            if kind in wanted:
                copy.wait_recv()

    def stream(x, still_z):
        fluid = solid[x] == 0
        for k in range(2):
            for i in range(19):
                c = VELOCITIES[i]
                if (c[2] == 0) != still_z:
                    continue
                rows = slice(T - c[1], T - c[1] + Y)
                read = post[k, SLOT[i], 1 + x - c[0], rows]
                if i:
                    edge = zpost[k, Z_PAIR[i], 1 + x - c[0], rows] if c[2] else None
                    read = shifted(read, edge, tuple(-a for a in c))
                    bounced = post[k, SLOT[OPPOSITE[i]], 1 + x, inner]
                    read = jnp.where(source[i, x] > 0.0, read, bounced)
                out[k, i, x] = jnp.where(fluid, read, pop[k, i, x])

    await2((0, 1, 0))
    for x in range(1, X - 1):
        stream(x, True)

    for copy in raw:
        copy.wait_recv()
    await2((1, 0, 0))
    for side in range(2):
        plane = 0 if side == 0 else X + 1
        sign = 1 if side == 0 else -1
        wanted = []
        for i in range(1, 19, 2):
            if VELOCITIES[i][0]:
                wanted.append((i, (sign * VELOCITIES[i][0],)))
        for k in range(2):
            rho = jnp.abs(psi[k, plane, inner]) * inv[k]
            u = [ghost[side, 3 * k + d] for d in range(3)]
            keep = 1.0 - inv[k]
            values = equilibrium(wanted, {w: rho * w for w in sorted(set(WEIGHTS))}, u)
            for i in values:
                value = values[i]
                if abs(keep) > 1e-9:
                    value = value + keep * post[k, SLOT[i], plane, inner]
                post[k, SLOT[i], plane, inner] = value
    await2((1, 1, 0))
    for x in (0, X - 1):
        stream(x, True)
    await2((0, 0, 1), (0, 1, 1))

    def came2(x, y, z, h):
        return recv2[Z_INDEX[(-x, -y, -z)], h]

    def put2(tile, k, g, x, t, plane, rows):
        zpost[k, g, plane, rows] = pltpu.roll(tile, (LANES - 2 * combo2(k, g, x, t) - 1) % LANES, 1)

    for h in range(2):
        merged = jnp.where(even, came2(0, 0, -1, h), came2(0, 0, 1, h))
        for x in range(h * half, (h + 1) * half):
            for k in range(2):
                for g in range(5):
                    for t in range(YT):
                        row = T * (1 + t)
                        put2(merged, k, g, x, t, 1 + x, slice(row, row + T))
    def edges2(along_x):
        for i in range(1, 19):
            c = VELOCITIES[i]
            if c[2] == 0 or not c[0 if along_x else 1]:
                continue
            g = Z_PAIR[i]
            for k in range(2):
                if c[0]:
                    x = X - 1 if c[0] > 0 else 0
                    plane = 0 if c[0] > 0 else X + 1
                    for t in range(YT):
                        row = T * (1 + t)
                        put2(came2(-c[0], 0, -c[2], x // half), k, g, x, t, plane, slice(row, row + T))
                else:
                    t = YT - 1 if c[1] > 0 else 0
                    rows = low_halo if c[1] > 0 else high_halo
                    for x in range(X):
                        put2(came2(0, -c[1], -c[2], x // half), k, g, x, t, 1 + x, rows)

    edges2(False)
    for x in range(1, X - 1):
        stream(x, False)
    await2((1, 0, 1))
    edges2(True)
    for x in (0, X - 1):
        stream(x, False)
    for copy in list(copies1.values()) + raw + copies2:
        copy.wait_send()


def body(populations, solid):
    X, Y, Z = solid.shape
    f32 = jnp.float32
    dma = pltpu.SemaphoreType.DMA
    return pl.pallas_call(
        step_kernel,
        out_shape=pltpu.VMEM(populations.shape, f32),
        in_specs=[pl.BlockSpec(memory_space=pl.ANY)] * 2,
        out_specs=pl.BlockSpec(memory_space=pltpu.VMEM),
        scratch_shapes=[
            pltpu.VMEM(populations.shape, f32),
            pltpu.VMEM(solid.shape, jnp.int32),
            pltpu.VMEM((2, X + 2, Y + 2 * T, Z), f32),
            pltpu.VMEM((2, X + 2, Y + 2 * T, Z), f32),
            pltpu.VMEM((2, 19, X + 2, Y + 2 * T, Z), f32),
            pltpu.VMEM((2, 5, X + 2, Y + 2 * T, Z), f32),
            pltpu.VMEM((3, X, Y, Z), f32),
            pltpu.VMEM((19, X, Y, Z), f32),
            pltpu.VMEM((T, LANES), f32),
            pltpu.VMEM((10, T, LANES), f32),
            pltpu.VMEM((2, T, LANES), f32),
            pltpu.VMEM((10, 2, T, LANES), f32),
            pltpu.VMEM((2, 6, Y, Z), f32),
            pltpu.VMEM((2, 6, Y, Z), f32),
            dma((X + 1,)),
            dma((28,)),
            dma((28,)),
            dma((26,)),
            dma((26,)),
        ],
        compiler_params=pltpu.CompilerParams(collective_id=0, has_side_effects=True),
    )(populations, solid)


def solution(mesh):
    in_specs = (P(None, None, "gx", "gy", "gz"), P("gx", "gy", "gz"))
    out_specs = P(None, None, "gx", "gy", "gz")
    return jax.shard_map(body, mesh=mesh, in_specs=in_specs, out_specs=out_specs, check_vma=False)
```

```python
import jax
import jax.numpy as jnp
from jax import lax
from jax.experimental import pallas as pl
from jax.experimental.pallas import tpu as pltpu
from jax.sharding import PartitionSpec as P

VELOCITIES = [
    (0, 0, 0),
    (1, 0, 0),
    (-1, 0, 0),
    (0, 1, 0),
    (0, -1, 0),
    (0, 0, 1),
    (0, 0, -1),
    (1, 1, 0),
    (-1, -1, 0),
    (1, -1, 0),
    (-1, 1, 0),
    (1, 0, 1),
    (-1, 0, -1),
    (1, 0, -1),
    (-1, 0, 1),
    (0, 1, 1),
    (0, -1, -1),
    (0, 1, -1),
    (0, -1, 1),
]
WEIGHTS = [1.0 / 3.0] + [1.0 / 18.0] * 6 + [1.0 / 36.0] * 12
OPPOSITE = [0, 2, 1, 4, 3, 6, 5, 8, 7, 10, 9, 12, 11, 14, 13, 16, 15, 18, 17]
COUPLING = 0.9
RELAX = (1.0, 0.8)
WALL = (0.3, 1.5)
AXES = ("gx", "gy", "gz")
MESH = pl.DeviceIdType.MESH

ORDER = (
    [0]
    + [i for i in range(19) if VELOCITIES[i][0] == 1]
    + [i for i in range(19) if VELOCITIES[i][0] == -1]
    + [i for i in range(1, 19) if VELOCITIES[i][0] == 0]
)
SLOT = {i: s for s, i in enumerate(ORDER)}
Z_UP = [i for i in range(19) if VELOCITIES[i][2] == 1]
Z_PAIR = {}
for _g, _i in enumerate(Z_UP):
    Z_PAIR[_i] = _g
    Z_PAIR[OPPOSITE[_i]] = _g
Z_OFFSETS = [v for v in VELOCITIES if v[2] != 0]
Z_INDEX = {v: n for n, v in enumerate(Z_OFFSETS)}
T = 8
LANES = 128


def step_kernel(pop_hbm, solid_hbm, out, pop, solid, psi, zpsi, post, zpost, vel, source,
                pack1, recv1, pack2, recv2, face, ghost, load_sem, send1, got1, send2, got2):
    X, Y, Z = solid.shape
    YT = Y // T
    lo, hi = slice(T, 2 * T), slice(Y, Y + T)
    low_halo, high_halo = slice(0, T), slice(Y + T, Y + 2 * T)
    inner = slice(T, Y + T)

    loads = [pltpu.make_async_copy(solid_hbm, solid, load_sem.at[X])]
    loads += [
        pltpu.make_async_copy(pop_hbm.at[:, :, x], pop.at[:, :, x], load_sem.at[x])
        for x in range(X)
    ]

    me = [lax.axis_index(a) for a in AXES]
    count = [lax.axis_size(a) for a in AXES]

    def device(offset):
        return tuple(lax.rem(me[d] + offset[d] + count[d], count[d]) for d in range(3))

    barrier = pltpu.get_barrier_semaphore()
    greeted = sorted(VELOCITIES[1:], key=lambda v: (-abs(v[2]), -abs(v[0]), -abs(v[1])))
    for offset in greeted:
        pl.semaphore_signal(barrier, inc=1, device_id=device(offset), device_id_type=MESH)
    for copy in loads:
        copy.start()

    lane = lax.broadcasted_iota(jnp.int32, (T, LANES), 1)
    pair = lane // 2
    lane_y = lax.broadcasted_iota(jnp.int32, (Y, LANES), 1)
    first, last = lane_y == 0, lane_y == Z - 1

    loads[0].wait()
    inv = [1.0 / t for t in RELAX]
    packed = jnp.zeros((T, LANES), jnp.float32)

    def combo1(k, x, t):
        return (k * X + x) * YT + t

    for x in range(X):
        loads[1 + x].wait()
        fluid = solid[x] == 0
        total, mom = [], [[], [], []]
        for k in range(2):
            f = [pop[k, i, x] for i in range(19)]
            rho = f[0]
            m = [None, None, None]
            for i in range(1, 19, 2):
                rho = rho + (f[i] + f[i + 1])
                diff = f[i] - f[i + 1]
                for d in range(3):
                    c = VELOCITIES[i][d]
                    if c:
                        m[d] = (
                            (diff if c > 0 else -diff)
                            if m[d] is None
                            else (m[d] + diff if c > 0 else m[d] - diff)
                        )
            total.append(rho)
            signed = jnp.where(fluid, rho, -WALL[k])
            psi[k, 1 + x, inner] = signed
            for d in range(3):
                mom[d].append(m[d] * inv[k] if inv[k] != 1.0 else m[d])
            for t in range(YT):
                j = combo1(k, x, t)
                piece = pltpu.roll(signed[t * T:(t + 1) * T], (2 * j + 1) % LANES, 1)
                packed = jnp.where(pair == j, piece, packed)
        scale = 1.0 / (total[0] * inv[0] + total[1] * inv[1])
        for d in range(3):
            vel[d, x] = (mom[d][0] + mom[d][1]) * scale
    pack1[...] = packed

    pl.semaphore_wait(barrier, len(greeted))

    def remote(src, dst, send, recv, n, offset):
        return pltpu.make_async_remote_copy(
            src_ref=src,
            dst_ref=dst,
            send_sem=send.at[n],
            recv_sem=recv.at[n],
            device_id=device(offset),
            device_id_type=MESH,
        )

    def edge_of(offset):
        dx, dy, _ = offset
        src_x = slice(1, X + 1) if dx == 0 else (slice(X, X + 1) if dx > 0 else slice(1, 2))
        dst_x = slice(1, X + 1) if dx == 0 else (slice(0, 1) if dx > 0 else slice(X + 1, X + 2))
        src_y = inner if dy == 0 else (hi if dy > 0 else lo)
        dst_y = inner if dy == 0 else (low_halo if dy > 0 else high_halo)
        return (src_x, src_y), (dst_x, dst_y)

    order = sorted(range(1, 19), key=lambda i: -sum(abs(c) for c in VELOCITIES[i][::2]))
    copies1 = {}
    for offset in sorted(greeted, key=lambda v: (-abs(v[2]), -abs(v[0]), -abs(v[1]))):
        n = len(copies1)
        if offset[2]:
            copy = remote(pack1, recv1.at[Z_INDEX[offset]], send1, got1, n, offset)
        else:
            s, d = edge_of(offset)
            copy = remote(psi.at[:, s[0], s[1]], psi.at[:, d[0], d[1]], send1, got1, n, offset)
        copy.start()
        copies1[offset] = copy
    raw = []
    for side in (1, -1):
        for i in range(19):
            if VELOCITIES[i][0] == side:
                src_plane, dst_plane = (X - 1, 0) if side > 0 else (0, X + 1)
                copy = remote(pop.at[1, i, src_plane], post.at[1, SLOT[i], dst_plane, inner],
                              send1, got1, 18 + len(raw), (side, 0, 0))
                copy.start()
                raw.append(copy)
    for dz in (1, -1):
        copies1[(0, 0, dz)].wait_recv()
    for offset in greeted:
        if offset[:2] != (0, 0) and not (offset[0] and offset[2]):
            copies1[offset].wait_recv()

    def came1(x, y, z):
        return recv1[Z_INDEX[(-x, -y, -z)]]

    def put1(merged, k, x, t, plane, rows):
        zpsi[k, plane, rows] = pltpu.roll(merged, (LANES - 2 * combo1(k, x, t) - 1) % LANES, 1)

    even = lane % 2 == 0

    def unpack1(dx, dy):
        merged = jnp.where(even, came1(dx, dy, -1), came1(dx, dy, 1))
        xs = range(X) if dx == 0 else ([X - 1] if dx < 0 else [0])
        ts = range(YT) if dy == 0 else ([YT - 1] if dy < 0 else [0])
        for k in range(2):
            for x in xs:
                for t in ts:
                    plane = 1 + x + dx * X
                    row = T * (1 + t + dy * YT)
                    put1(merged, k, x, t, plane, slice(row, row + T))

    for dx, dy in ((0, 0), (0, -1), (0, 1)):
        unpack1(dx, dy)

    def shifted(base, edge, move):
        if move[2] == 0:
            return base
        if move[2] > 0:
            return pltpu.roll(jnp.where(first, edge, base), Z - 1, 1)
        return pltpu.roll(jnp.where(last, edge, base), 1, 1)

    half = X // 2

    def combo2(k, g, x, t):
        return (((x % half) * 2 + k) * 5 + g) * YT + t

    def equilibrium(pairs, rho_of, u):
        flat = 1.0 - 1.5 * (u[0] * u[0] + u[1] * u[1] + u[2] * u[2])
        result = {}
        for i, signs in pairs:
            if i == 0:
                result[0] = rho_of[WEIGHTS[0]] * flat
                continue
            along = None
            for d in range(3):
                c = VELOCITIES[i][d]
                if c:
                    along = (
                        (u[d] if c > 0 else -u[d])
                        if along is None
                        else (along + u[d] if c > 0 else along - u[d])
                    )
            w = rho_of[WEIGHTS[i]]
            even_part = w * (flat + 4.5 * (along * along))
            odd_part = w * (3.0 * along)
            if 1 in signs:
                result[i] = even_part + odd_part
            if -1 in signs:
                result[i + 1] = even_part - odd_part
        return result

    everything = [(0, (1,))] + [(i, (1, -1)) for i in range(1, 19, 2)]
    copies2 = []
    kinds = []

    def launch2(src, dst, offset):
        copy = remote(src, dst, send2, got2, len(copies2), offset)
        copy.start()
        copies2.append(copy)
        kinds.append(tuple(abs(c) for c in offset))

    packs = [jnp.zeros((T, LANES), jnp.float32) for _ in range(2)]
    for x in list(range(1, X - 1)) + [0, X - 1]:
        if x == 0:
            for dx in (1, -1):
                for dz in (1, -1):
                    copies1[(dx, 0, dz)].wait_recv()
            for dx in (1, -1):
                unpack1(dx, 0)
        grads = []
        for k in range(2):
            parts = [None, None, None]
            beside = {}
            for i in range(1, 19):
                c = VELOCITIES[i]
                at = (k, 1 + x + c[0], slice(T + c[1], T + c[1] + Y))
                value = shifted(psi[at], zpsi[at] if c[2] else None, c)
                if k == 0:
                    source[OPPOSITE[i], x] = value
                beside[i] = jnp.abs(value)
            for i in range(1, 19, 2):
                term = WEIGHTS[i] * (beside[i] - beside[i + 1])
                for d in range(3):
                    c = VELOCITIES[i][d]
                    if c:
                        parts[d] = (
                            (term if c > 0 else -term)
                            if parts[d] is None
                            else (parts[d] + term if c > 0 else parts[d] - term)
                        )
            grads.append(parts)
        for k in range(2):
            u = [vel[d, x] - (COUPLING * RELAX[k]) * grads[1 - k][d] for d in range(3)]
            rho = jnp.abs(psi[k, 1 + x, inner]) * inv[k]
            keep = 1.0 - inv[k]
            values = equilibrium(everything, {w: rho * w for w in sorted(set(WEIGHTS))}, u)
            for i in range(19):
                if abs(keep) > 1e-9:
                    values[i] = values[i] + keep * pop[k, i, x]
                post[k, SLOT[i], 1 + x, inner] = values[i]
            if x in (0, X - 1):
                for d in range(3):
                    face[int(x != 0), 3 * k + d] = u[d]
            for g, i in enumerate(Z_UP):
                ends = jnp.where(last, values[i], values[OPPOSITE[i]])
                for t in range(YT):
                    j = combo2(k, g, x, t)
                    piece = pltpu.roll(ends[t * T:(t + 1) * T], (2 * j + 1) % LANES, 1)
                    packs[x // half] = jnp.where(pair == j, piece, packs[x // half])
        if x in (0, X - 1):
            side = int(x != 0)
            launch2(face.at[side], ghost.at[1 - side], (2 * side - 1, 0, 0))
    for h in range(2):
        pack2[h] = packs[h]

    for i in order:
        offset = VELOCITIES[i]
        if offset[2]:
            halves = slice(0, 2) if offset[0] == 0 else (slice(1, 2) if offset[0] > 0 else slice(0, 1))
            launch2(pack2.at[halves], recv2.at[Z_INDEX[offset], halves], offset)
            continue
        s, d = edge_of(offset)
        if offset[0] and offset[1]:
            launch2(post.at[:, SLOT[i], s[0], s[1]], post.at[:, SLOT[i], d[0], d[1]], offset)
        elif offset[1]:
            for q in range(19):
                if VELOCITIES[q][1] == offset[1]:
                    launch2(post.at[:, SLOT[q], s[0], s[1]], post.at[:, SLOT[q], d[0], d[1]], offset)

    def await2(*wanted):
        for copy, kind in zip(copies2, kinds):
            if kind in wanted:
                copy.wait_recv()

    def stream(x, still_z):
        fluid = solid[x] == 0
        for k in range(2):
            for i in range(19):
                c = VELOCITIES[i]
                if (c[2] == 0) != still_z:
                    continue
                rows = slice(T - c[1], T - c[1] + Y)
                read = post[k, SLOT[i], 1 + x - c[0], rows]
                if i:
                    edge = zpost[k, Z_PAIR[i], 1 + x - c[0], rows] if c[2] else None
                    read = shifted(read, edge, tuple(-a for a in c))
                    bounced = post[k, SLOT[OPPOSITE[i]], 1 + x, inner]
                    read = jnp.where(source[i, x] > 0.0, read, bounced)
                out[k, i, x] = jnp.where(fluid, read, pop[k, i, x])

    await2((0, 1, 0))
    for x in range(1, X - 1):
        stream(x, True)

    for copy in raw:
        copy.wait_recv()
    await2((1, 0, 0))
    for side in range(2):
        plane = 0 if side == 0 else X + 1
        sign = 1 if side == 0 else -1
        wanted = []
        for i in range(1, 19, 2):
            if VELOCITIES[i][0]:
                wanted.append((i, (sign * VELOCITIES[i][0],)))
        for k in range(2):
            rho = jnp.abs(psi[k, plane, inner]) * inv[k]
            u = [ghost[side, 3 * k + d] for d in range(3)]
            keep = 1.0 - inv[k]
            values = equilibrium(wanted, {w: rho * w for w in sorted(set(WEIGHTS))}, u)
            for i in values:
                value = values[i]
                if abs(keep) > 1e-9:
                    value = value + keep * post[k, SLOT[i], plane, inner]
                post[k, SLOT[i], plane, inner] = value
    await2((1, 1, 0))
    for x in (0, X - 1):
        stream(x, True)
    await2((0, 0, 1), (0, 1, 1))

    def came2(x, y, z, h):
        return recv2[Z_INDEX[(-x, -y, -z)], h]

    def put2(tile, k, g, x, t, plane, rows):
        zpost[k, g, plane, rows] = pltpu.roll(tile, (LANES - 2 * combo2(k, g, x, t) - 1) % LANES, 1)

    for h in range(2):
        merged = jnp.where(even, came2(0, 0, -1, h), came2(0, 0, 1, h))
        for x in range(h * half, (h + 1) * half):
            for k in range(2):
                for g in range(5):
                    for t in range(YT):
                        row = T * (1 + t)
                        put2(merged, k, g, x, t, 1 + x, slice(row, row + T))
    def edges2(along_x):
        for i in range(1, 19):
            c = VELOCITIES[i]
            if c[2] == 0 or not c[0 if along_x else 1]:
                continue
            g = Z_PAIR[i]
            for k in range(2):
                if c[0]:
                    x = X - 1 if c[0] > 0 else 0
                    plane = 0 if c[0] > 0 else X + 1
                    for t in range(YT):
                        row = T * (1 + t)
                        put2(came2(-c[0], 0, -c[2], x // half), k, g, x, t, plane, slice(row, row + T))
                else:
                    t = YT - 1 if c[1] > 0 else 0
                    rows = low_halo if c[1] > 0 else high_halo
                    for x in range(X):
                        put2(came2(0, -c[1], -c[2], x // half), k, g, x, t, 1 + x, rows)

    edges2(False)
    for x in range(1, X - 1):
        stream(x, False)
    await2((1, 0, 1))
    edges2(True)
    for x in (0, X - 1):
        stream(x, False)
    for copy in list(copies1.values()) + raw + copies2:
        copy.wait_send()


def body(populations, solid):
    X, Y, Z = solid.shape
    f32 = jnp.float32
    dma = pltpu.SemaphoreType.DMA
    return pl.pallas_call(
        step_kernel,
        out_shape=pltpu.VMEM(populations.shape, f32),
        in_specs=[pl.BlockSpec(memory_space=pl.ANY)] * 2,
        out_specs=pl.BlockSpec(memory_space=pltpu.VMEM),
        scratch_shapes=[
            pltpu.VMEM(populations.shape, f32),
            pltpu.VMEM(solid.shape, jnp.int32),
            pltpu.VMEM((2, X + 2, Y + 2 * T, Z), f32),
            pltpu.VMEM((2, X + 2, Y + 2 * T, Z), f32),
            pltpu.VMEM((2, 19, X + 2, Y + 2 * T, Z), f32),
            pltpu.VMEM((2, 5, X + 2, Y + 2 * T, Z), f32),
            pltpu.VMEM((3, X, Y, Z), f32),
            pltpu.VMEM((19, X, Y, Z), f32),
            pltpu.VMEM((T, LANES), f32),
            pltpu.VMEM((10, T, LANES), f32),
            pltpu.VMEM((2, T, LANES), f32),
            pltpu.VMEM((10, 2, T, LANES), f32),
            pltpu.VMEM((2, 6, Y, Z), f32),
            pltpu.VMEM((2, 6, Y, Z), f32),
            dma((X + 1,)),
            dma((28,)),
            dma((28,)),
            dma((26,)),
            dma((26,)),
        ],
        compiler_params=pltpu.CompilerParams(collective_id=0, has_side_effects=True),
    )(populations, solid)


def solution(mesh):
    in_specs = (P(None, None, "gx", "gy", "gz"), P("gx", "gy", "gz"))
    out_specs = P(None, None, "gx", "gy", "gz")
    return jax.shard_map(body, mesh=mesh, in_specs=in_specs, out_specs=out_specs, check_vma=False)
```
